32 devices in a mesh: row: 16 (over z, x, core), head: 2 (over y).
Axes of the slice: x: 2, y: 2, z: 4, core: 2. Of those that a mesh axis runs over, the one named last changes fastest.
Arguments:
- sequence_matrix: float32 [32, 512, 256], P('row', 'head'), may hold values from -6 to 6
- pair_representation: float32 [512, 512, 128], P('row', 'head'), may hold values from -6 to 6
- alignment_row_mask: int32 [32], P('row'), may hold values 0 or 1
- residue_mask: int32 [512], replicated, may hold values 0 or 1
- attention_scale_vector: float32 [256], replicated, may hold values from 0.1 to 1.9
- asking_factor_matrix: float32 [256, 256], replicated, may hold values from -0.375 to 0.375
- lookup_factor_matrix: float32 [256, 256], replicated, may hold values from -0.375 to 0.375
- content_factor_matrix: float32 [256, 256], replicated, may hold values from -0.375 to 0.375
- sigmoid_factor_matrix: float32 [256, 256], replicated, may hold values from -0.375 to 0.375
- final_factor_matrix: float32 [256, 256], replicated, may hold values from -0.375 to 0.375
- pair_norm_gain: float32 [128], replicated, may hold values from 0.1 to 1.9
- bias_weight: float32 [128, 8], replicated, may hold values from -20 to 20
- tensor_scale_vector: float32 [256], replicated, may hold values from 0.1 to 1.9
- first_factor_matrix: float32 [256, 32], replicated, may hold values from -0.375 to 0.375
- second_factor_matrix: float32 [256, 32], replicated, may hold values from -0.375 to 0.375
- outer_weight: float32 [1024, 128], replicated, may hold values from -1 to 1
Outputs:
- msa_out: float32 [32, 512, 256], P('row', 'head')
- pair_out: float32 [512, 512, 128], P('row', 'head')
The draws below stay inside these ranges and needn't reach their ends.
All inputs are finite; a program needn't handle non-finite values. No bound on the sum of `alignment_row_mask` on one device may be relied on, other than what follows from the above.
Results may differ from the reference program's by a relative error of at most 0.0003.
Values sent between devices are 32-bit elements; how exact they have to be, the bound alone decides.
A program may use at most 128 MiB of HBM per device.

```python
import math
import jax
import jax.numpy as jnp
from jax import lax

FEATURE_DEPTH = 256
C_Z = 128
ATTENTION_GROUPS = 8
TENSOR_FACTOR = 32
CROP_LENGTH = 512
SEQUENCE_TOTAL = 32
N_ROW = 16


def draw_bias_weight(key, part):
    normal_draw = jnp.clip(jax.random.normal(key, (C_Z, ATTENTION_GROUPS), jnp.float32), -4.0, 4.0)
    return normal_draw / math.sqrt(C_Z)


def touch_ends(drawn, own_key, least, high):
    spot = [jax.random.randint(jax.random.fold_in(own_key, axis), (), 0, length) for axis, length in enumerate(drawn.shape)]
    longest = drawn.shape.index(max(drawn.shape))
    beside = spot[:longest] + [(spot[longest] + 1) % drawn.shape[longest]] + spot[longest + 1:]
    return drawn.at[tuple(spot)].set(least).at[tuple(beside)].set(high)


def levels(stream_key, shape, pieces, smallest, top_value):
    def one(axis_at, blocks):
        steps = jax.random.uniform(jax.random.fold_in(jax.random.fold_in(stream_key, 6), axis_at), (blocks,), jnp.float32, smallest / len(pieces), top_value / len(pieces))
        return jnp.repeat(jnp.exp(steps), shape[axis_at] // blocks).reshape((-1,) + (1,) * (len(shape) - axis_at - 1))

    gain = one(*pieces[0])
    for cut in pieces[1:]:
        gain = gain * one(*cut)
    return gain


def noise(stream_key, dims, scale, bound, shards=(), held_as=jnp.bfloat16):
    factor_of = levels(stream_key, dims, shards, -0.22, 0.18) if shards else 1.0
    entries = jax.random.normal(stream_key, dims, jnp.float32) * scale * factor_of
    return jnp.minimum(jnp.maximum(entries, -bound), bound).astype(held_as)


def setup_inputs(seed: int = 0) -> dict:
    seeds = jax.random.split(jax.random.key(seed), 17)
    sequence_matrix = noise(seeds[0], (SEQUENCE_TOTAL, CROP_LENGTH, FEATURE_DEPTH), 1.0, 6.0, ((0, 16), (1, 2)), jnp.float32)
    pair_representation = noise(seeds[1], (CROP_LENGTH, CROP_LENGTH, C_Z), 1.0, 6.0, ((0, 16), (1, 2)), jnp.float32)
    alignment_row_mask = touch_ends((jax.random.randint(seeds[2], (SEQUENCE_TOTAL,), 0, 4) < 3).astype(jnp.int32), jax.random.fold_in(seeds[2], 1), 0, 1)
    residue_mask = touch_ends((jax.random.randint(seeds[3], (CROP_LENGTH,), 0, 8) < 7).astype(jnp.int32), jax.random.fold_in(seeds[3], 1), 0, 1)
    attention_scale_vector = jnp.clip(1.0 + 0.18 * jax.random.normal(seeds[4], (FEATURE_DEPTH,), jnp.float32), 0.1, 1.9)
    asking_factor_matrix = noise(seeds[5], (FEATURE_DEPTH, FEATURE_DEPTH), FEATURE_DEPTH ** -0.5, 0.375, (), jnp.float32)
    lookup_factor_matrix = noise(seeds[6], (FEATURE_DEPTH, FEATURE_DEPTH), FEATURE_DEPTH ** -0.5, 0.375, (), jnp.float32)
    content_factor_matrix = noise(seeds[7], (FEATURE_DEPTH, FEATURE_DEPTH), FEATURE_DEPTH ** -0.5, 0.375, (), jnp.float32)
    sigmoid_factor_matrix = noise(seeds[8], (FEATURE_DEPTH, FEATURE_DEPTH), FEATURE_DEPTH ** -0.5, 0.375, (), jnp.float32)
    final_factor_matrix = noise(seeds[9], (FEATURE_DEPTH, FEATURE_DEPTH), FEATURE_DEPTH ** -0.5, 0.375, (), jnp.float32)
    pair_norm_gain = jnp.clip(1.0 + 0.18 * jax.random.normal(seeds[10], (C_Z,), jnp.float32), 0.1, 1.9)
    bias_weight = draw_bias_weight(jax.random.fold_in(seeds[16], 71), 0)
    tensor_scale_vector = jnp.clip(1.0 + 0.18 * jax.random.normal(seeds[12], (FEATURE_DEPTH,), jnp.float32), 0.1, 1.9)
    first_factor_matrix = noise(seeds[13], (FEATURE_DEPTH, TENSOR_FACTOR), FEATURE_DEPTH ** -0.5, 0.375, (), jnp.float32)
    second_factor_matrix = noise(seeds[14], (FEATURE_DEPTH, TENSOR_FACTOR), FEATURE_DEPTH ** -0.5, 0.375, (), jnp.float32)
    outer_weight = noise(seeds[15], (TENSOR_FACTOR * TENSOR_FACTOR, C_Z), TENSOR_FACTOR ** -0.5, 1.0, (), jnp.float32)
    return dict(sequence_matrix=sequence_matrix, pair_representation=pair_representation, alignment_row_mask=alignment_row_mask, residue_mask=residue_mask, attention_scale_vector=attention_scale_vector, asking_factor_matrix=asking_factor_matrix, lookup_factor_matrix=lookup_factor_matrix, content_factor_matrix=content_factor_matrix, sigmoid_factor_matrix=sigmoid_factor_matrix, final_factor_matrix=final_factor_matrix, pair_norm_gain=pair_norm_gain, bias_weight=bias_weight, tensor_scale_vector=tensor_scale_vector, first_factor_matrix=first_factor_matrix, second_factor_matrix=second_factor_matrix, outer_weight=outer_weight)


exact_arithmetic = lax.Precision.HIGHEST

def apply_layer_norm(values, gains):
    center = values - lax.optimization_barrier(jnp.mean(values, axis=-1, keepdims=True))
    spread = lax.optimization_barrier(jnp.mean(center * center, axis=-1, keepdims=True))
    return center * lax.rsqrt(spread + 1e-05) * gains

def reference(sequence_matrix, pair_representation, alignment_row_mask, residue_mask, attention_scale_vector, asking_factor_matrix, lookup_factor_matrix, content_factor_matrix, sigmoid_factor_matrix, final_factor_matrix, pair_norm_gain, bias_weight, tensor_scale_vector, first_factor_matrix, second_factor_matrix, outer_weight):
    split_groups = FEATURE_DEPTH // ATTENTION_GROUPS
    pair_norm = apply_layer_norm(pair_representation, pair_norm_gain)
    bias_all = jnp.einsum('ijc,ch->hij', pair_norm, bias_weight, precision=exact_arithmetic)
    key_bias = (residue_mask.astype(jnp.float32) - 1.0) * 1000000000.0
    stacked_blocks = jnp.stack([asking_factor_matrix, lookup_factor_matrix, content_factor_matrix, sigmoid_factor_matrix], axis=1)
    inv_root = 1.0 / math.sqrt(split_groups)

    def attend_rows(sequence_features):
        normalized_rows = apply_layer_norm(sequence_features, attention_scale_vector)
        projected_rows = jnp.einsum('ic,cfe->ife', normalized_rows, stacked_blocks, precision=exact_arithmetic).reshape(CROP_LENGTH, 4, ATTENTION_GROUPS, split_groups)
        logits = jnp.einsum('ihd,jhd->hij', projected_rows[:, 0], projected_rows[:, 1], precision=exact_arithmetic) * inv_root + bias_all + key_bias
        largest = lax.optimization_barrier(jnp.max(logits, axis=-1, keepdims=True))
        exponent = jnp.exp(logits - largest)
        weights = exponent / lax.optimization_barrier(jnp.sum(exponent, axis=-1, keepdims=True))
        attended = jnp.einsum('hij,jhd->ihd', weights, projected_rows[:, 2], precision=exact_arithmetic)
        sigmoid_scaled = attended * jax.nn.sigmoid(projected_rows[:, 3])
        return sequence_features + jnp.dot(sigmoid_scaled.reshape(CROP_LENGTH, FEATURE_DEPTH), final_factor_matrix, precision=exact_arithmetic)
    alignment_updated = lax.map(attend_rows, sequence_matrix)
    outer_product_norm = apply_layer_norm(alignment_updated, tensor_scale_vector)
    res_live = residue_mask.astype(jnp.float32)
    live = alignment_row_mask.astype(jnp.float32)[:, None] * res_live[None, :]
    left_side = jnp.einsum('sic,co->sio', outer_product_norm, first_factor_matrix, precision=exact_arithmetic) * live[..., None]
    right = jnp.einsum('sic,co->sio', outer_product_norm, second_factor_matrix, precision=exact_arithmetic) * live[..., None]
    count = jnp.sum(alignment_row_mask.astype(jnp.float32))
    row_block_slice = CROP_LENGTH // N_ROW
    left_side_blocks = left_side.reshape(SEQUENCE_TOTAL, N_ROW, row_block_slice, TENSOR_FACTOR).transpose(1, 0, 2, 3)
    live_blocks = res_live.reshape(N_ROW, row_block_slice)

    def outer_block(inputs):
        left_part, live_part = inputs
        outer = jnp.einsum('sic,sjd->ijcd', left_part, right, precision=exact_arithmetic).reshape(row_block_slice, CROP_LENGTH, TENSOR_FACTOR * TENSOR_FACTOR)
        pair_update = jnp.einsum('ijk,kz->ijz', outer, outer_weight, precision=exact_arithmetic)
        norm_function = count * live_part[:, None] * res_live[None, :] + 0.001
        return pair_update / norm_function[..., None]
    pair_updates = lax.map(outer_block, (left_side_blocks, live_blocks)).reshape(CROP_LENGTH, CROP_LENGTH, C_Z)
    return (alignment_updated, pair_representation + pair_updates)
```

```python
import functools
import math

import jax
import jax.numpy as jnp
from jax import lax
from jax.experimental import pallas as pl
from jax.experimental.pallas import tpu as pltpu
from jax.sharding import PartitionSpec as P


HIGH = lax.Precision.HIGHEST


def apply_layer_norm(values, gains):
    center = values - jnp.mean(values, axis=-1, keepdims=True)
    spread = jnp.mean(center * center, axis=-1, keepdims=True)
    return center * lax.rsqrt(spread + 1e-05) * gains


def split(x):
    hi = x.astype(jnp.bfloat16)
    lo = (x - hi.astype(jnp.float32)).astype(jnp.bfloat16)
    return hi, lo


def mm(a, b, dims=(((1,), (0,)), ((), ()))):
    return lax.dot_general(a, b, dims, preferred_element_type=jnp.float32)


def split_outside(x):
    hi = lax.reduce_precision(x, 8, 7)
    return hi.astype(jnp.bfloat16), lax.reduce_precision(x - hi, 8, 7).astype(jnp.bfloat16)


NT = (((1,), (1,)), ((), ()))


def bias_kernel(pair_ref, gain_ref, weight_ref, out_ref):
    rows, cols, width = pair_ref.shape
    w_hi, w_lo = split(weight_ref[...])
    heads = w_hi.shape[0]
    w_both = jnp.concatenate([w_hi, w_lo], axis=0)
    for r in range(rows):
        x = apply_layer_norm(pair_ref[r], gain_ref[...])
        x_hi, x_lo = split(x)
        both = mm(w_both, x_hi, NT)
        out_ref[r] = both[:heads] + both[heads:] + mm(w_hi, x_lo, NT)


def pair_bias(pair, gain, weight):
    rows, cols, width = pair.shape
    heads = weight.shape[1]
    step = 4
    return pl.pallas_call(
        bias_kernel,
        grid=(rows // step,),
        in_specs=[
            pl.BlockSpec((step, cols, width), lambda i: (i, 0, 0)),
            pl.BlockSpec((1, width), lambda i: (0, 0)),
            pl.BlockSpec((heads, width), lambda i: (0, 0)),
        ],
        out_specs=pl.BlockSpec((step, heads, cols), lambda i: (i, 0, 0)),
        out_shape=jax.ShapeDtypeStruct((rows, heads, cols), jnp.float32),
        cost_estimate=pl.CostEstimate(flops=10**9, bytes_accessed=5 * 10**6, transcendentals=0),
    )(pair, gain[None, :], weight.T)


def attend_kernel(q_ref, k_ref, v_ref, bias_ref, key_ref, out_ref):
    blocks, heads, depth, keys = bias_ref.shape
    n_rows = q_ref.shape[0]
    width = v_ref.shape[3] // 2
    key_bias = key_ref[...]
    for s in range(n_rows):
        pieces = []
        for h in range(heads):
            logits = mm(q_ref[s, h], k_ref[s, h], NT)
            logits = logits + bias_ref[:, h].reshape(blocks * depth, keys) + key_bias
            largest = jnp.max(logits, axis=-1, keepdims=True)
            e = jnp.exp(logits - largest)
            total = jnp.sum(e, axis=-1, keepdims=True)
            e_hi, e_lo = split(e)
            v = v_ref[s, h]
            both = mm(e_hi, v)
            got = both[:, :width] + both[:, width:] + mm(e_lo, v[:, :width])
            pieces.append(got / total)
        out_ref[s] = jnp.concatenate(pieces, axis=-1)


def attend(q, k, v, bias, key_bias):
    n_rows, heads, residues, packed = q.shape
    groups, _, depth, keys = bias.shape
    width = v.shape[3] // 2
    blocks = max(1, 128 // depth)
    steps = groups // blocks
    rows = blocks * depth
    return pl.pallas_call(
        attend_kernel,
        grid=(steps,),
        in_specs=[
            pl.BlockSpec((n_rows, heads, rows, packed), lambda i: (0, 0, i, 0)),
            pl.BlockSpec((n_rows, heads, keys, packed), lambda i: (0, 0, 0, 0)),
            pl.BlockSpec((n_rows, heads, keys, 2 * width), lambda i: (0, 0, 0, 0)),
            pl.BlockSpec((blocks, heads, depth, keys), lambda i: (i, 0, 0, 0)),
            pl.BlockSpec((1, keys), lambda i: (0, 0)),
        ],
        out_specs=pl.BlockSpec((n_rows, rows, heads * width), lambda i: (0, i, 0)),
        out_shape=jax.ShapeDtypeStruct((n_rows, residues, heads * width), jnp.float32),
        cost_estimate=pl.CostEstimate(flops=4 * 10**9, bytes_accessed=6 * 10**6, transcendentals=2 * 10**6),
    )(q, k, v, bias, key_bias)


def outer_kernel(scale_ref, left_ref, weight_ref, right_ref, live_ref, pair_ref, out_ref,
                 r_hi, r_lo, t_hi, t_lo):
    step, cols, depth = pair_ref.shape
    rows_all = r_hi.shape[1]
    n_rows = left_ref.shape[0] // step
    width = rows_all // n_rows
    me = pl.program_id(0)

    @pl.when(me == 0)
    def _():
        hi, lo = split(right_ref[...].T)
        r_hi[...] = hi
        r_lo[...] = lo

    left = left_ref[...]
    group = 2
    for d0 in range(0, width, group):
        t = mm(left, weight_ref[:, d0 * depth:(d0 + group) * depth])
        hi, lo = split(t)
        for g in range(group):
            d = d0 + g
            for i in range(step):
                src = (slice(i * n_rows, (i + 1) * n_rows), slice(g * depth, (g + 1) * depth))
                dst = (slice(d * n_rows, (d + 1) * n_rows), slice(i * depth, (i + 1) * depth))
                t_hi[dst] = hi[src]
                t_lo[dst] = lo[src]
    update = mm(r_hi[...], t_hi[...]) + mm(r_lo[...], t_hi[...]) + mm(r_hi[...], t_lo[...])
    for i in range(step):
        norm = scale_ref[me * step + i] * live_ref[...] + 0.001
        out_ref[i] = pair_ref[i] + update[:, i * depth:(i + 1) * depth] / norm


def outer_mean(scale, left, weight, right, live, pair):
    rows, cols, depth = pair.shape
    total = right.shape[0]
    n_rows = left.shape[0] // rows
    packed = left.shape[1]
    step = 4
    return pl.pallas_call(
        outer_kernel,
        grid=(rows // step,),
        in_specs=[
            pl.BlockSpec(memory_space=pltpu.SMEM),
            pl.BlockSpec((step * n_rows, packed), lambda i: (i, 0)),
            pl.BlockSpec(weight.shape, lambda i: (0, 0)),
            pl.BlockSpec(right.shape, lambda i: (0, 0)),
            pl.BlockSpec((cols, 1), lambda i: (0, 0)),
            pl.BlockSpec((step, cols, depth), lambda i: (i, 0, 0)),
        ],
        out_specs=pl.BlockSpec((step, cols, depth), lambda i: (i, 0, 0)),
        out_shape=jax.ShapeDtypeStruct(pair.shape, jnp.float32),
        scratch_shapes=[
            pltpu.VMEM((cols, total), jnp.bfloat16),
            pltpu.VMEM((cols, total), jnp.bfloat16),
            pltpu.VMEM((total, step * depth), jnp.bfloat16),
            pltpu.VMEM((total, step * depth), jnp.bfloat16),
        ],
        cost_estimate=pl.CostEstimate(flops=9 * 10**9, bytes_accessed=10**7, transcendentals=0),
    )(scale, left, weight, right, live, pair)


def around(n):
    return [[(src, (src + k) % n) for src in range(n)] for k in range(n)]


def gather_heads(block, n, index, axis):
    size = block.shape[axis]
    shape = list(block.shape)
    shape[axis] = size * n
    whole = jnp.zeros(shape, block.dtype)
    for k in range(n):
        part = block if k == 0 else lax.ppermute(block, "head", around(n)[k])
        whole = lax.dynamic_update_slice_in_dim(whole, part, ((index - k) % n) * size, axis)
    return whole


def exchange_heads(block, n, index, split_axis, concat_axis):
    size = block.shape[split_axis] // n
    shape = list(block.shape)
    shape[split_axis] = size
    length = shape[concat_axis]
    shape[concat_axis] = length * n
    whole = jnp.zeros(shape, block.dtype)
    for k in range(n):
        part = lax.dynamic_slice_in_dim(block, ((index + k) % n) * size, size, split_axis)
        if k:
            part = lax.ppermute(part, "head", around(n)[k])
        whole = lax.dynamic_update_slice_in_dim(whole, part, ((index - k) % n) * length, concat_axis)
    return whole


def body(
    sequence_matrix,
    pair_representation,
    alignment_row_mask,
    residue_mask,
    attention_scale_vector,
    asking_factor_matrix,
    lookup_factor_matrix,
    content_factor_matrix,
    sigmoid_factor_matrix,
    final_factor_matrix,
    pair_norm_gain,
    bias_weight,
    tensor_scale_vector,
    first_factor_matrix,
    second_factor_matrix,
    outer_weight,
):
    head_count = lax.axis_size("head")
    head_index = lax.axis_index("head")
    row_index = lax.axis_index("row")
    n_rows, col_count, width = sequence_matrix.shape
    residues = col_count * head_count
    pair_rows = pair_representation.shape[0]
    pair_depth = pair_representation.shape[2]
    heads_all = bias_weight.shape[1]
    head_width = width // heads_all
    local_heads = heads_all // head_count
    local_width = local_heads * head_width
    opm_width = first_factor_matrix.shape[1]

    sequence_all = gather_heads(sequence_matrix, head_count, head_index, 1)

    bias_all = pair_bias(pair_representation, pair_norm_gain, bias_weight)
    bias_part = exchange_heads(
        bias_all.transpose(1, 0, 2), head_count, head_index, 0, 2
    )
    bias = lax.all_gather(bias_part, "row", axis=0, tiled=False)
    key_bias = ((residue_mask.astype(jnp.float32) - 1.0) * 1000000000.0)[None, :]

    norm_all = apply_layer_norm(sequence_all, attention_scale_vector)

    def local(weight):
        mine = lax.dynamic_slice_in_dim(weight, head_index * local_width, local_width, 1)
        made = jnp.einsum("sic,ce->sie", norm_all, mine, precision=HIGH)
        return made.reshape(n_rows, residues, local_heads, head_width).transpose(0, 2, 1, 3)

    q_hi, q_lo = split_outside(local(asking_factor_matrix) * (1.0 / math.sqrt(head_width)))
    k_hi, k_lo = split_outside(local(lookup_factor_matrix))
    v_hi, v_lo = split_outside(local(content_factor_matrix))
    attended = attend(
        jnp.concatenate([q_hi, q_hi, q_lo], axis=-1),
        jnp.concatenate([k_hi, k_lo, k_hi], axis=-1),
        jnp.concatenate([v_hi, v_lo], axis=-1),
        bias,
        key_bias,
    )
    norm_mine = apply_layer_norm(sequence_matrix, attention_scale_vector)
    gate = jax.nn.sigmoid(
        jnp.einsum("sic,ce->sie", norm_mine, sigmoid_factor_matrix, precision=HIGH)
    )
    returned_values = exchange_heads(attended, head_count, head_index, 1, 2) * gate
    alignment_updated = sequence_matrix + jnp.einsum(
        "jna,ab->jnb", returned_values, final_factor_matrix, precision=HIGH
    )

    outer_product_norm = apply_layer_norm(alignment_updated, tensor_scale_vector)
    live_cols = lax.dynamic_slice_in_dim(residue_mask, head_index * col_count, col_count).astype(
        jnp.float32
    )
    row_live = alignment_row_mask.astype(jnp.float32)
    live = row_live[:, None] * live_cols[None, :]
    left_side = (
        jnp.einsum("sic,co->soi", outer_product_norm, first_factor_matrix, precision=HIGH)
        * live[:, None, :]
    )
    right = (
        jnp.einsum("sic,co->soi", outer_product_norm, second_factor_matrix, precision=HIGH)
        * live[:, None, :]
    )
    carried = jnp.broadcast_to(row_live[:, None, None], (n_rows, 1, col_count))
    right_all = lax.all_gather(
        jnp.concatenate([right, carried], axis=1), "row", axis=0, tiled=True
    )
    left_all = gather_heads(left_side, head_count, head_index, 2)
    left_mine = lax.all_to_all(left_all, "row", split_axis=2, concat_axis=0, tiled=True)
    count = jnp.sum(right_all[:, opm_width, 0])
    total_rows = right_all.shape[0]
    right_rows = right_all[:, :opm_width].transpose(1, 0, 2).reshape(
        opm_width * total_rows, col_count
    )
    left_rows = left_mine.transpose(2, 0, 1).reshape(pair_rows * total_rows, opm_width)
    l_hi, l_lo = split_outside(left_rows)
    w_hi, w_lo = split_outside(outer_weight.reshape(opm_width, opm_width * pair_depth))
    rows_live = lax.dynamic_slice_in_dim(residue_mask, row_index * pair_rows, pair_rows).astype(
        jnp.float32
    )
    pair_out = outer_mean(
        count * rows_live,
        jnp.concatenate([l_hi, l_hi, l_lo], axis=1),
        jnp.concatenate([w_hi, w_lo, w_hi], axis=0),
        right_rows,
        live_cols[:, None],
        pair_representation,
    )
    return alignment_updated, pair_out


def solution(mesh):
    placed = (P("row", "head", None), P("row", "head", None), P("row")) + (P(),) * 13
    return jax.shard_map(
        body,
        mesh=mesh,
        in_specs=placed,
        out_specs=(P("row", "head", None), P("row", "head", None)),
        check_vma=False,
    )
```

```python
import functools
import math

import jax
import jax.numpy as jnp
from jax import lax
from jax.experimental import pallas as pl
from jax.experimental.pallas import tpu as pltpu
from jax.sharding import PartitionSpec as P


HIGH = lax.Precision.HIGHEST


def apply_layer_norm(values, gains):
    center = values - jnp.mean(values, axis=-1, keepdims=True)
    spread = jnp.mean(center * center, axis=-1, keepdims=True)
    return center * lax.rsqrt(spread + 1e-05) * gains


def split(x):
    hi = x.astype(jnp.bfloat16)
    lo = (x - hi.astype(jnp.float32)).astype(jnp.bfloat16)
    return hi, lo


def mm(a, b, dims=(((1,), (0,)), ((), ()))):
    return lax.dot_general(a, b, dims, preferred_element_type=jnp.float32)


def split_outside(x):
    hi = lax.reduce_precision(x, 8, 7)
    return hi.astype(jnp.bfloat16), lax.reduce_precision(x - hi, 8, 7).astype(jnp.bfloat16)


NT = (((1,), (1,)), ((), ()))


def bias_kernel(pair_ref, gain_ref, weight_ref, out_ref):
    rows, cols, width = pair_ref.shape
    w_hi, w_lo = split(weight_ref[...])
    heads = w_hi.shape[0]
    w_both = jnp.concatenate([w_hi, w_lo], axis=0)
    for r in range(rows):
        x = apply_layer_norm(pair_ref[r], gain_ref[...])
        x_hi, x_lo = split(x)
        both = mm(w_both, x_hi, NT)
        out_ref[r] = both[:heads] + both[heads:] + mm(w_hi, x_lo, NT)


def pair_bias(pair, gain, weight):
    rows, cols, width = pair.shape
    heads = weight.shape[1]
    step = 4
    return pl.pallas_call(
        bias_kernel,
        grid=(rows // step,),
        in_specs=[
            pl.BlockSpec((step, cols, width), lambda i: (i, 0, 0)),
            pl.BlockSpec((1, width), lambda i: (0, 0)),
            pl.BlockSpec((heads, width), lambda i: (0, 0)),
        ],
        out_specs=pl.BlockSpec((step, heads, cols), lambda i: (i, 0, 0)),
        out_shape=jax.ShapeDtypeStruct((rows, heads, cols), jnp.float32),
        cost_estimate=pl.CostEstimate(flops=10**9, bytes_accessed=5 * 10**6, transcendentals=0),
    )(pair, gain[None, :], weight.T)


def attend_kernel(x_ref, gain_ref, w_ref, bias_ref, key_ref, out_ref, q_ref, k_ref, v_ref):
    blocks, heads, depth, keys = bias_ref.shape
    n_rows = x_ref.shape[0]
    width = v_ref.shape[3] // 2
    local = heads * width
    rows = blocks * depth
    step = pl.program_id(0)

    @pl.when(step == 0)
    def _():
        w_hi, w_lo = split(w_ref[...])
        for s in range(n_rows):
            x_hi, x_lo = split(apply_layer_norm(x_ref[s], gain_ref[...]))
            made = mm(x_hi, w_hi) + mm(x_lo, w_hi) + mm(x_hi, w_lo)
            q_hi, q_lo = split(made[:, :local] * (1.0 / math.sqrt(width)))
            k_hi, k_lo = split(made[:, local:2 * local])
            v_hi, v_lo = split(made[:, 2 * local:])
            for h in range(heads):
                at = slice(h * width, (h + 1) * width)
                q_ref[s, h] = jnp.concatenate([q_hi[:, at], q_hi[:, at], q_lo[:, at]], axis=-1)
                k_ref[s, h] = jnp.concatenate([k_hi[:, at], k_lo[:, at], k_hi[:, at]], axis=-1)
                v_ref[s, h] = jnp.concatenate([v_hi[:, at], v_lo[:, at]], axis=-1)

    key_bias = key_ref[...]
    mine = pl.ds(pl.multiple_of(step * rows, rows), rows)
    for s in range(n_rows):
        pieces = []
        for h in range(heads):
            logits = mm(q_ref[s, h, mine, :], k_ref[s, h], NT)
            logits = logits + bias_ref[:, h].reshape(rows, keys) + key_bias
            largest = jnp.max(logits, axis=-1, keepdims=True)
            e = jnp.exp(logits - largest)
            total = jnp.sum(e, axis=-1, keepdims=True)
            e_hi, e_lo = split(e)
            v = v_ref[s, h]
            both = mm(e_hi, v)
            got = both[:, :width] + both[:, width:] + mm(e_lo, v[:, :width])
            pieces.append(got / total)
        out_ref[s] = jnp.concatenate(pieces, axis=-1)


def attend(x, gain, weight, bias, key_bias):
    n_rows, residues, features = x.shape
    groups, heads, depth, keys = bias.shape
    local = weight.shape[1] // 3
    width = local // heads
    blocks = max(1, 128 // depth)
    rows = blocks * depth
    return pl.pallas_call(
        attend_kernel,
        grid=(groups // blocks,),
        in_specs=[
            pl.BlockSpec(x.shape, lambda i: (0, 0, 0)),
            pl.BlockSpec((1, features), lambda i: (0, 0)),
            pl.BlockSpec(weight.shape, lambda i: (0, 0)),
            pl.BlockSpec((blocks, heads, depth, keys), lambda i: (i, 0, 0, 0)),
            pl.BlockSpec((1, keys), lambda i: (0, 0)),
        ],
        out_specs=pl.BlockSpec((n_rows, rows, local), lambda i: (0, i, 0)),
        out_shape=jax.ShapeDtypeStruct((n_rows, residues, local), jnp.float32),
        scratch_shapes=[
            pltpu.VMEM((n_rows, heads, residues, 3 * width), jnp.bfloat16),
            pltpu.VMEM((n_rows, heads, residues, 3 * width), jnp.bfloat16),
            pltpu.VMEM((n_rows, heads, residues, 2 * width), jnp.bfloat16),
        ],
        cost_estimate=pl.CostEstimate(flops=4 * 10**9, bytes_accessed=6 * 10**6, transcendentals=2 * 10**6),
    )(x, gain[None, :], weight, bias, key_bias)


def outer_kernel(scale_ref, left_ref, weight_ref, right_ref, live_ref, pair_ref, out_ref,
                 r_hi, r_lo, t_hi, t_lo):
    step, cols, depth = pair_ref.shape
    rows_all = r_hi.shape[1]
    n_rows = left_ref.shape[0] // step
    width = rows_all // n_rows
    me = pl.program_id(0)

    @pl.when(me == 0)
    def _():
        hi, lo = split(right_ref[...].T)
        r_hi[...] = hi
        r_lo[...] = lo

    left = left_ref[...]
    group = 2
    for d0 in range(0, width, group):
        t = mm(left, weight_ref[:, d0 * depth:(d0 + group) * depth])
        hi, lo = split(t)
        for g in range(group):
            d = d0 + g
            for i in range(step):
                src = (slice(i * n_rows, (i + 1) * n_rows), slice(g * depth, (g + 1) * depth))
                dst = (slice(d * n_rows, (d + 1) * n_rows), slice(i * depth, (i + 1) * depth))
                t_hi[dst] = hi[src]
                t_lo[dst] = lo[src]
    update = mm(r_hi[...], t_hi[...]) + mm(r_lo[...], t_hi[...]) + mm(r_hi[...], t_lo[...])
    for i in range(step):
        norm = scale_ref[me * step + i] * live_ref[...] + 0.001
        out_ref[i] = pair_ref[i] + update[:, i * depth:(i + 1) * depth] / norm


def outer_mean(scale, left, weight, right, live, pair):
    rows, cols, depth = pair.shape
    total = right.shape[0]
    n_rows = left.shape[0] // rows
    packed = left.shape[1]
    step = 4
    return pl.pallas_call(
        outer_kernel,
        grid=(rows // step,),
        in_specs=[
            pl.BlockSpec(memory_space=pltpu.SMEM),
            pl.BlockSpec((step * n_rows, packed), lambda i: (i, 0)),
            pl.BlockSpec(weight.shape, lambda i: (0, 0)),
            pl.BlockSpec(right.shape, lambda i: (0, 0)),
            pl.BlockSpec((cols, 1), lambda i: (0, 0)),
            pl.BlockSpec((step, cols, depth), lambda i: (i, 0, 0)),
        ],
        out_specs=pl.BlockSpec((step, cols, depth), lambda i: (i, 0, 0)),
        out_shape=jax.ShapeDtypeStruct(pair.shape, jnp.float32),
        scratch_shapes=[
            pltpu.VMEM((cols, total), jnp.bfloat16),
            pltpu.VMEM((cols, total), jnp.bfloat16),
            pltpu.VMEM((total, step * depth), jnp.bfloat16),
            pltpu.VMEM((total, step * depth), jnp.bfloat16),
        ],
        cost_estimate=pl.CostEstimate(flops=9 * 10**9, bytes_accessed=10**7, transcendentals=0),
    )(scale, left, weight, right, live, pair)


def gather_kernel(n, block_ref, out_ref, own_sem, send_sem, recv_sem):
    me = lax.axis_index("row")
    core = me % 2
    x = (me // 2) % 2
    nz = n // 4
    z = me // 4

    def place(zz, xx, cc):
        return (zz * 2 + xx) * 2 + cc

    barrier = pltpu.get_barrier_semaphore()
    up_ok, down_ok = z + 1 < nz, z >= 1

    def greet(target):
        pl.semaphore_signal(barrier, inc=1, device_id={"row": target},
                            device_id_type=pl.DeviceIdType.MESH)

    greet(place(z, x, 1 - core))
    greet(place(z, 1 - x, core))
    pl.when(up_ok)(lambda: greet(place(z + 1, x, core)))
    pl.when(down_ok)(lambda: greet(place(z - 1, x, core)))
    peers = 2 + jnp.where(up_ok, 1, 0) + jnp.where(down_ok, 1, 0)
    pl.semaphore_wait(barrier, peers)

    own = pltpu.make_async_copy(block_ref, out_ref.at[me], own_sem)
    own.start()

    def sends(d, other):
        found = []
        first = core == 0
        if other == 0:
            cross = (z >= 0) if d == 0 else jnp.logical_not(first)
            run = z >= 0
        else:
            cross = None
            run = first
        if d <= 0:
            found.append((jnp.logical_and(run, up_ok), 0, lambda: place(z + 1, x, core)))
        if d >= 0:
            found.append((jnp.logical_and(run, down_ok), 1, lambda: place(z - 1, x, core)))
        if cross is not None:
            found.append((cross, 2, lambda: place(z, 1 - x, core)))
        found.append((z >= 0, 3, lambda: place(z, x, 1 - core)))
        return found

    def copy(source, kind, target, mine):
        return pltpu.make_async_remote_copy(
            src_ref=block_ref if mine else out_ref.at[source],
            dst_ref=out_ref.at[source],
            send_sem=send_sem.at[kind, source],
            recv_sem=recv_sem.at[source],
            device_id={"row": target},
            device_id_type=pl.DeviceIdType.MESH,
        )

    hops = [(0, 0), (0, 1)]
    for far in range(1, nz):
        hops += [(-far, 0), (far, 0), (-far, 1), (far, 1)]

    def each(action):
        for d, other in hops:
            source = place(z + d, (x + other) % 2, core)
            mine = d == 0 and other == 0
            there = jnp.logical_and(z + d >= 0, z + d < nz)

            @pl.when(there)
            def _(d=d, other=other, source=source, mine=mine):
                action(d, other, source, mine)

    def forward(d, other, source, mine):
        if not mine:
            copy(source, 3, place(z, x, 1 - core), False).wait_recv()
        for ok, kind, target in sends(d, other):
            pl.when(ok)(lambda kind=kind, target=target: copy(source, kind, target(), mine).start())

    def finish(d, other, source, mine):
        for ok, kind, target in sends(d, other):
            pl.when(ok)(lambda kind=kind, target=target: copy(source, kind, target(), mine).wait_send())

    each(forward)
    for k in range(n // 2):
        copy(2 * k + 1 - core, 3, place(z, x, 1 - core), False).wait_recv()
    each(finish)
    own.wait()


def gather_rows(block, n, ident):
    return pl.pallas_call(
        functools.partial(gather_kernel, n),
        out_shape=jax.ShapeDtypeStruct((n,) + block.shape, block.dtype),
        in_specs=[pl.BlockSpec(memory_space=pltpu.VMEM)],
        out_specs=pl.BlockSpec(memory_space=pl.ANY),
        scratch_shapes=[
            pltpu.SemaphoreType.DMA,
            pltpu.SemaphoreType.DMA((4, n)),
            pltpu.SemaphoreType.DMA((n,)),
        ],
        compiler_params=pltpu.CompilerParams(collective_id=ident, has_side_effects=True),
    )(block)


def around(n):
    return [[(src, (src + k) % n) for src in range(n)] for k in range(n)]


def gather_heads(block, n, index, axis):
    size = block.shape[axis]
    shape = list(block.shape)
    shape[axis] = size * n
    whole = jnp.zeros(shape, block.dtype)
    for k in range(n):
        part = block if k == 0 else lax.ppermute(block, "head", around(n)[k])
        whole = lax.dynamic_update_slice_in_dim(whole, part, ((index - k) % n) * size, axis)
    return whole


def exchange_heads(block, n, index, split_axis, concat_axis):
    size = block.shape[split_axis] // n
    shape = list(block.shape)
    shape[split_axis] = size
    length = shape[concat_axis]
    shape[concat_axis] = length * n
    whole = jnp.zeros(shape, block.dtype)
    for k in range(n):
        part = lax.dynamic_slice_in_dim(block, ((index + k) % n) * size, size, split_axis)
        if k:
            part = lax.ppermute(part, "head", around(n)[k])
        whole = lax.dynamic_update_slice_in_dim(whole, part, ((index - k) % n) * length, concat_axis)
    return whole


def body(
    sequence_matrix,
    pair_representation,
    alignment_row_mask,
    residue_mask,
    attention_scale_vector,
    asking_factor_matrix,
    lookup_factor_matrix,
    content_factor_matrix,
    sigmoid_factor_matrix,
    final_factor_matrix,
    pair_norm_gain,
    bias_weight,
    tensor_scale_vector,
    first_factor_matrix,
    second_factor_matrix,
    outer_weight,
):
    head_count = lax.axis_size("head")
    head_index = lax.axis_index("head")
    row_index = lax.axis_index("row")
    row_count = lax.axis_size("row")
    n_rows, col_count, width = sequence_matrix.shape
    residues = col_count * head_count
    pair_rows = pair_representation.shape[0]
    pair_depth = pair_representation.shape[2]
    heads_all = bias_weight.shape[1]
    head_width = width // heads_all
    local_heads = heads_all // head_count
    local_width = local_heads * head_width
    opm_width = first_factor_matrix.shape[1]

    sequence_all = gather_heads(sequence_matrix, head_count, head_index, 1)

    bias_all = pair_bias(pair_representation, pair_norm_gain, bias_weight)
    bias_part = exchange_heads(
        bias_all.transpose(1, 0, 2), head_count, head_index, 0, 2
    )
    bias = gather_rows(bias_part, row_count, 0)
    key_bias = ((residue_mask.astype(jnp.float32) - 1.0) * 1000000000.0)[None, :]

    weights = jnp.concatenate(
        [
            lax.dynamic_slice_in_dim(w, head_index * local_width, local_width, 1)
            for w in (asking_factor_matrix, lookup_factor_matrix, content_factor_matrix)
        ],
        axis=1,
    )
    attended = attend(sequence_all, attention_scale_vector, weights, bias, key_bias)
    norm_mine = apply_layer_norm(sequence_matrix, attention_scale_vector)
    gate = jax.nn.sigmoid(
        jnp.einsum("sic,ce->sie", norm_mine, sigmoid_factor_matrix, precision=HIGH)
    )
    returned_values = exchange_heads(attended, head_count, head_index, 1, 2) * gate
    alignment_updated = sequence_matrix + jnp.einsum(
        "jna,ab->jnb", returned_values, final_factor_matrix, precision=HIGH
    )

    outer_product_norm = apply_layer_norm(alignment_updated, tensor_scale_vector)
    live_cols = lax.dynamic_slice_in_dim(residue_mask, head_index * col_count, col_count).astype(
        jnp.float32
    )
    row_live = alignment_row_mask.astype(jnp.float32)
    live = row_live[:, None] * live_cols[None, :]
    left_side = (
        jnp.einsum("sic,co->soi", outer_product_norm, first_factor_matrix, precision=HIGH)
        * live[:, None, :]
    )
    right = (
        jnp.einsum("sic,co->soi", outer_product_norm, second_factor_matrix, precision=HIGH)
        * live[:, None, :]
    )
    left_all = gather_heads(left_side, head_count, head_index, 1)
    carried = jnp.broadcast_to(row_live[:, None, None], (n_rows, 8, col_count))
    sides = gather_rows(jnp.concatenate([left_all, right, carried], axis=1), row_count, 1)
    sides = sides.reshape(row_count * n_rows, -1, col_count)
    left_width = head_count * opm_width
    first_row = row_index * pair_rows
    left_mine = lax.dynamic_slice(
        sides,
        (0, (first_row // col_count) * opm_width, first_row % col_count),
        (row_count * n_rows, opm_width, pair_rows),
    )
    right_all = sides[:, left_width:]
    total_rows = row_count * n_rows
    count = jnp.sum(right_all[:, opm_width, 0])
    right_rows = right_all[:, :opm_width].transpose(1, 0, 2).reshape(
        opm_width * total_rows, col_count
    )
    left_rows = left_mine.transpose(2, 0, 1).reshape(pair_rows * total_rows, opm_width)
    l_hi, l_lo = split_outside(left_rows)
    w_hi, w_lo = split_outside(outer_weight.reshape(opm_width, opm_width * pair_depth))
    rows_live = lax.dynamic_slice_in_dim(residue_mask, row_index * pair_rows, pair_rows).astype(
        jnp.float32
    )
    pair_out = outer_mean(
        count * rows_live,
        jnp.concatenate([l_hi, l_hi, l_lo], axis=1),
        jnp.concatenate([w_hi, w_lo, w_hi], axis=0),
        right_rows,
        live_cols[:, None],
        pair_representation,
    )
    return alignment_updated, pair_out


def solution(mesh):
    placed = (P("row", "head", None), P("row", "head", None), P("row")) + (P(),) * 13
    return jax.shard_map(
        body,
        mesh=mesh,
        in_specs=placed,
        out_specs=(P("row", "head", None), P("row", "head", None)),
        check_vma=False,
    )
```
